32 devices in a mesh: dp: 16 (over z, y, x), mp: 2 (over core).
Axes of the slice: x: 2, y: 2, z: 4, core: 2. Of those that a mesh axis runs over, the one named last changes fastest.
Arguments:
- clean: float32 [64, 3, 4096], P(('dp', 'mp')), may hold values from -1 to 1
- noise: float32 [64, 3, 4096], P(('dp', 'mp')), may hold values from -12 to 12
- lowres: float32 [64, 3, 4096], P(('dp', 'mp')), may hold values from -1 to 1
- aug_noise: float32 [64, 3, 4096], P(('dp', 'mp')), may hold values from -5 to 5
- timesteps: int32 [64], P(('dp', 'mp')), may hold values from 0 to 999
- aug_levels: int32 [64], P(('dp', 'mp')), may hold values from 0 to 999
- lengths: int32 [64], P(('dp', 'mp')), may hold values from 1 to 128
- text: bfloat16 [64, 128, 4096], P(('dp', 'mp')), may hold values from -160 to 160
- w_stem: float32 [6, 128], replicated, may hold values from -2.5 to 2.5
- w_time: float32 [256, 256], replicated, may hold values from -0.375 to 0.375
- conv_one: bfloat16 [1152, 128], replicated, may hold values from -0.1875 to 0.1875
- conv_two: bfloat16 [1152, 128], replicated, may hold values from -0.1875 to 0.1875
- kv_weight: bfloat16 [4096, 256], P('mp'), may hold values from -0.09375 to 0.09375
- w_query: bfloat16 [128, 128], replicated, may hold values from -0.5 to 0.5
- w_output: bfloat16 [128, 128], replicated, may hold values from -0.5 to 0.5
- w_head: bfloat16 [3, 128], replicated, may hold values from -0.5 to 0.5
Outputs:
- conv_one_update: float32 [1152, 128], P(('dp', 'mp'))
- conv_two_update: float32 [1152, 128], P(('dp', 'mp'))
- kv_update: float32 [4096, 256], P('mp', 'dp')
- loss_mean: float32 [], replicated
The draws below stay inside these ranges and needn't reach their ends.
All inputs are finite; a program needn't handle non-finite values.
Results may differ from the reference program's by a relative error of at most 0.03.
The reference program's roundings to bfloat16 on the way count: a program that leaves them out, or rounds other values in their place, can miss the bound.
Values may be sent and summed in bfloat16 or wider, within the bound.
A program may use at most 128 MiB of HBM per device.

```python
import math
import jax
import jax.numpy as jnp
from jax import lax

S = 64
C = 128
GROUPS = 32
HEADS = 2
HEAD_DIM = 64
A = 128
L = 128
DT = 4096
FREQS = 64
STEPS = 1000
BATCH = 64


def draw_text(key, part):
    base = jax.random.normal(jax.random.fold_in(key, 11), (BATCH, L, DT), jnp.float32)
    base = jnp.clip(base, -4.0, 4.0)
    return base.astype(jnp.bfloat16)


def draw_noise(key, part):
    ramp = jnp.arange(BATCH, dtype=jnp.float32) / max(BATCH - 1, 1)
    spread = (1.0 + 2.0 * ramp)[:, None, None]
    base = jnp.clip(jax.random.normal(jax.random.fold_in(key, 22), (BATCH, 3, S * S), jnp.float32), -4.0, 4.0)
    return (base * spread).astype(jnp.float32)


def set_ends(entries, stream_key, least, high):
    longest = entries.shape.index(max(entries.shape))
    spots = []
    for shift in (0, 1):
        where = [jax.random.randint(jax.random.fold_in(stream_key, axis), (), 0, length) for axis, length in enumerate(entries.shape)]
        where[longest] = (where[longest] + shift) % entries.shape[longest]
        spots.append(tuple(where))
    return entries.at[spots[0]].set(least).at[spots[1]].set(high)


def steps_of(rng, extent, cuts, low, largest):
    def one(axis_at, shards_of):
        steps = jax.random.uniform(jax.random.fold_in(jax.random.fold_in(rng, 6), axis_at), (shards_of,), jnp.float32, low / len(cuts), largest / len(cuts))
        return jnp.repeat(jnp.exp(steps), extent[axis_at] // shards_of).reshape((-1,) + (1,) * (len(extent) - axis_at - 1))

    gain = one(*cuts[0])
    for cut in cuts[1:]:
        gain = gain * one(*cut)
    return gain


def gaussian(stream_key, extent, scale, limit, cuts=(), kind=jnp.bfloat16):
    values = scale * jax.random.normal(stream_key, extent, jnp.float32)
    if cuts:
        values = values * steps_of(stream_key, extent, cuts, -0.22, 0.18)
    return jnp.clip(values, -limit, limit).astype(kind)


def setup_inputs(seed: int = 0) -> dict:
    arg_keys = jax.random.split(jax.random.key(seed), 17)
    clean = jnp.clip(jax.random.uniform(arg_keys[0], (BATCH, 3, S * S), jnp.float32, -1.0, 1.0) * steps_of(arg_keys[0], (BATCH, 3, S * S), ((0, 32),), -0.4, 0.0), -1.0, 1.0)
    noise = draw_noise(jax.random.fold_in(arg_keys[16], 71), 0)
    lowres = jnp.clip(jax.random.uniform(arg_keys[2], (BATCH, 3, S * S), jnp.float32, -1.0, 1.0) * steps_of(arg_keys[2], (BATCH, 3, S * S), ((0, 32),), -0.4, 0.0), -1.0, 1.0)
    aug_noise = gaussian(arg_keys[3], (BATCH, 3, S * S), 1.0, 5.0, ((0, 32),), jnp.float32)
    timesteps = set_ends(jax.random.randint(arg_keys[4], (BATCH,), 0, STEPS), jax.random.fold_in(arg_keys[4], 1), 0, STEPS - 1).astype(jnp.int32)
    aug_levels = set_ends(jax.random.randint(arg_keys[5], (BATCH,), 0, STEPS), jax.random.fold_in(arg_keys[5], 1), 0, STEPS - 1).astype(jnp.int32)
    lengths = set_ends(jax.random.randint(arg_keys[6], (BATCH,), 1, L + 1), jax.random.fold_in(arg_keys[6], 1), 1, L).astype(jnp.int32)
    text = draw_text(jax.random.fold_in(arg_keys[16], 71), 0)
    w_stem = gaussian(arg_keys[8], (6, C), 6 ** -0.5, 2.5, (), jnp.float32)
    w_time = gaussian(arg_keys[9], (4 * FREQS, 2 * C), (4 * FREQS) ** -0.5, 0.375, (), jnp.float32)
    conv_one = gaussian(arg_keys[10], (9 * C, C), (9 * C) ** -0.5, 0.1875)
    conv_two = gaussian(arg_keys[11], (9 * C, C), (9 * C) ** -0.5, 0.1875)
    kv_weight = gaussian(arg_keys[12], (DT, 2 * A), DT ** -0.5, 0.09375, ((0, 2),))
    w_query = gaussian(arg_keys[13], (C, A), C ** -0.5, 0.5)
    w_output = gaussian(arg_keys[14], (A, C), A ** -0.5, 0.5)
    w_head = gaussian(arg_keys[15], (3, C), C ** -0.5, 0.5)
    return dict(clean=clean, noise=noise, lowres=lowres, aug_noise=aug_noise, timesteps=timesteps, aug_levels=aug_levels, lengths=lengths, text=text, w_stem=w_stem, w_time=w_time, conv_one=conv_one, conv_two=conv_two, kv_weight=kv_weight, w_query=w_query, w_output=w_output, w_head=w_head)


def signal_level(index):
    ratio = (index.astype(jnp.float32) / STEPS + 0.008) / 1.008
    cosine = jnp.cos(ratio * (math.pi / 2.0))
    return cosine * cosine

def sinusoid(index):
    freqs = jnp.exp(-math.log(10000.0) * jnp.arange(FREQS, dtype=jnp.float32) / FREQS)
    angles = index.astype(jnp.float32) * freqs
    return jnp.concatenate([jnp.sin(angles), jnp.cos(angles)])

def prepare(clean, noise, lowres, aug_noise, tstep, level, w_stem, w_time):
    signal = signal_level(tstep)
    aug_signal = signal_level(level)
    noisy = jnp.sqrt(signal) * clean + jnp.sqrt(1.0 - signal) * noise
    low_noisy = jnp.sqrt(aug_signal) * lowres + jnp.sqrt(1.0 - aug_signal) * aug_noise
    stacked = jnp.concatenate([noisy, low_noisy], axis=0)
    h_start = jnp.einsum('kp,kc->pc', stacked, w_stem, precision=lax.Precision.HIGHEST)
    feature = jnp.concatenate([sinusoid(tstep), sinusoid(level)])[None, :]
    embed = jax.nn.silu(jnp.dot(feature, w_time, precision=lax.Precision.HIGHEST))[0]
    channels = w_stem.shape[1]
    return (h_start, embed[:channels], embed[channels:])

def group_matrix(channels):
    members = channels // GROUPS
    labels = jnp.arange(channels) // members
    return (labels[:, None] == labels[None, :]).astype(jnp.float32) / members

def group_norm(values, grouping):
    average = jnp.dot(lax.optimization_barrier(jnp.mean(values, axis=0, keepdims=True)), grouping, precision=lax.Precision.HIGHEST)
    centred = values - average
    spread = jnp.dot(lax.optimization_barrier(jnp.mean(centred * centred, axis=0, keepdims=True)), grouping, precision=lax.Precision.HIGHEST)
    return centred * lax.rsqrt(spread + 1e-05)

def convolve(activation, weight):
    channels = weight.shape[1]
    kernel = weight.reshape(3, 3, channels, channels)
    picture = activation.reshape(1, S, S, channels)
    result = lax.conv_general_dilated(picture, kernel, (1, 1), 'SAME', dimension_numbers=('NHWC', 'HWIO', 'NHWC'), preferred_element_type=jnp.float32)
    return result.reshape(S * S, channels)

def image_loss(conv_one, conv_two, keys_values, h_start, scale, shift, keep, w_query, w_output, w_head, noise):
    channels = conv_one.shape[1]
    grouping = group_matrix(channels)
    act_one = jax.nn.silu(group_norm(h_start, grouping)).astype(jnp.bfloat16)
    conv_out_one = convolve(act_one, conv_one)
    act_two = jax.nn.silu(group_norm(conv_out_one, grouping) * (1.0 + scale) + shift).astype(jnp.bfloat16)
    h_mid = h_start + convolve(act_two, conv_two)
    normed = group_norm(h_mid, grouping).astype(jnp.bfloat16)
    queries = (jnp.dot(normed, w_query, preferred_element_type=jnp.float32) * HEAD_DIM ** (-0.5)).astype(jnp.bfloat16)
    width = w_query.shape[1]
    pieces = []
    for head_index in range(HEADS):
        lower = head_index * HEAD_DIM
        upper = lower + HEAD_DIM
        scores = jnp.dot(queries[:, lower:upper], keys_values[:, lower:upper].T, preferred_element_type=jnp.float32)
        scores = jnp.where(keep[None, :], scores, -1e+30)
        highest = lax.optimization_barrier(jnp.max(scores, axis=1, keepdims=True))
        weights = jnp.exp(scores - highest)
        probs = (weights / lax.optimization_barrier(jnp.sum(weights, axis=1, keepdims=True))).astype(jnp.bfloat16)
        pieces.append(jnp.dot(probs, keys_values[:, width + lower:width + upper], preferred_element_type=jnp.float32))
    attended = jnp.concatenate(pieces, axis=1).astype(jnp.bfloat16)
    h_out = h_mid + jnp.dot(attended, w_output, preferred_element_type=jnp.float32)
    pred = jnp.einsum('kc,pc->kp', w_head.astype(jnp.float32), h_out.astype(jnp.bfloat16).astype(jnp.float32))
    error = pred - noise
    return jnp.sum(error * error)

def normalize(grad):
    return grad * lax.rsqrt(jnp.mean(grad * grad) + 1e-06)

def reference(clean, noise, lowres, aug_noise, timesteps, aug_levels, lengths, text, w_stem, w_time, conv_one, conv_two, kv_weight, w_query, w_output, w_head):

    def visit(carry, items):
        grad_one, grad_two, grad_kv, total = carry
        clean_i, noise_i, low_i, aug_i, tstep, level, length, text_i = items
        h_start, scale, shift = prepare(clean_i, noise_i, low_i, aug_i, tstep, level, w_stem, w_time)
        keys_values = jnp.dot(text_i, kv_weight, preferred_element_type=jnp.float32).astype(jnp.bfloat16)
        keep = jnp.arange(text_i.shape[0]).astype(jnp.int32) < length
        value, pullback = jax.vjp(lambda first, second, third: image_loss(first, second, third, h_start, scale, shift, keep, w_query, w_output, w_head, noise_i), conv_one, conv_two, keys_values)
        part_one, part_two, part_kv = pullback(jnp.ones((), value.dtype))
        grad_kv = grad_kv + jnp.dot(text_i.T, part_kv, preferred_element_type=jnp.float32)
        return ((grad_one + part_one.astype(jnp.float32), grad_two + part_two.astype(jnp.float32), grad_kv, total + value), None)
    start = (jnp.zeros(conv_one.shape, jnp.float32), jnp.zeros(conv_two.shape, jnp.float32), jnp.zeros(kv_weight.shape, jnp.float32), jnp.zeros((), jnp.float32))
    finals, unused = lax.scan(visit, start, (clean, noise, lowres, aug_noise, timesteps, aug_levels, lengths, text))
    grad_one, grad_two, grad_kv, total = finals
    count = clean.shape[0] * clean.shape[1] * clean.shape[2]
    return (normalize(grad_one), normalize(grad_two), normalize(grad_kv), total / count)
```

```python
import functools
import math

import jax
import jax.numpy as jnp
from jax import lax
from jax.experimental import pallas as pl
from jax.experimental.pallas import tpu as pltpu
from jax.sharding import PartitionSpec as P

S = 64
GROUPS = 32
HEADS = 2
HEAD_DIM = 64
FREQS = 64
STEPS = 1000
F32 = jnp.float32
BF16 = jnp.bfloat16
EPS = 1e-05
TAPS = 3


def level_of(index):
    ratio = (index / STEPS + 0.008) / 1.008
    cosine = jnp.cos(ratio * (math.pi / 2.0))
    return cosine * cosine


def dot(a, b):
    return jnp.dot(a, b, preferred_element_type=F32)


def dot_lhs_t(a, b):
    return lax.dot_general(a, b, (((0,), (0,)), ((), ())), preferred_element_type=F32)


def dot_rhs_t(a, b):
    return lax.dot_general(a, b, (((1,), (1,)), ((), ())), preferred_element_type=F32)


def fold(values):
    rows, lanes = values.shape
    return jnp.sum(values.reshape(rows // 8, 8, lanes), axis=0)


def group_mean(acc, count):
    total = jnp.sum(acc, axis=0, keepdims=True)
    channels = acc.shape[1]
    total = jnp.broadcast_to(total, acc.shape)
    lane = lax.broadcasted_iota(jnp.int32, acc.shape, 1)
    members = channels // GROUPS
    step = 1
    while step < members:
        up = pltpu.roll(total, channels - step, 1)
        down = pltpu.roll(total, step, 1)
        total = total + jnp.where((lane // step) % 2 == 0, up, down)
        step *= 2
    return total[0:1] / (count * members)


def sigmoid(x):
    return 1.0 / (1.0 + jnp.exp(-x))


def split3(x):
    one = x.astype(BF16).astype(F32)
    two = (x - one).astype(BF16).astype(F32)
    three = (x - one - two).astype(BF16).astype(F32)
    return one, two, three


def radices_of(size):
    parts = []
    for step in (2, 2):
        if size % step == 0 and size > 1:
            parts.append(step)
            size //= step
    while size > 1:
        step = next((s for s in (4, 2, 3, 5, 7) if size % s == 0), size)
        parts.append(step)
        size //= step
    return tuple(parts)


def blocks_of(shape, radices):
    return [tuple(reversed(radices[j:])) + tuple(shape) for j in range(len(radices))]


def lands_of(shape, radices, dp_size, mp_size):
    lands = [(mp_size - 1, dp_size) + tuple(shape)]
    for j, radix in enumerate(radices):
        lands.append((radix - 1,) + tuple(reversed(radices[j + 1 :])) + tuple(shape))
    return lands


def scratch_of(shape, radices, dp_size, mp_size):
    copies = mp_size - 1 + sum(r - 1 for r in radices)
    return (
        [pltpu.VMEM(s, BF16) for s in blocks_of(shape, radices)]
        + [pltpu.VMEM(s, BF16) for s in lands_of(shape, radices, dp_size, mp_size)]
        + [pltpu.SemaphoreType.DMA((copies,)), pltpu.SemaphoreType.DMA((copies,))]
    )


class Scatter:
    def __init__(self, pick, read, final, radices, refs, dp_size, mp_size):
        k = len(radices)
        self.pick, self.read, self.final, self.radices = pick, read, final, radices
        self.sums, self.lands = refs[:k], refs[k : 2 * k + 1]
        self.send, self.recv = refs[2 * k + 1 :]
        self.dp_size, self.mp_size = dp_size, mp_size
        self.dp, self.mp = lax.axis_index("dp"), lax.axis_index("mp")
        self.place = []
        stride = 1
        for radix in radices:
            self.place.append((lax.rem(lax.div(self.dp, stride), radix), stride))
            stride *= radix

    def copies(self, j):
        out = []
        if j == 0:
            for k in range(self.mp_size - 1):
                peer = lax.rem(self.mp + k + 1, self.mp_size)
                out.append((self.pick(peer), self.lands[0].at[k], k, (self.dp, peer)))
        else:
            radix = self.radices[j - 1]
            digit, stride = self.place[j - 1]
            first = self.mp_size - 1 + sum(r - 1 for r in self.radices[: j - 1])
            rest = len(self.radices) - j
            for k in range(radix - 1):
                there = lax.rem(digit + k + 1, radix)
                src = self.sums[j - 1].at[(slice(None),) * rest + (there,)]
                peer = self.dp + (there - digit) * stride
                out.append((src, self.lands[j].at[k], first + k, (peer, self.mp)))
        return [
            pltpu.make_async_remote_copy(
                src_ref=src,
                dst_ref=dst,
                send_sem=self.send.at[sem],
                recv_sem=self.recv.at[sem],
                device_id=peer,
                device_id_type=pl.DeviceIdType.MESH,
            )
            for src, dst, sem, peer in out
        ]

    def start(self, j):
        for copy in self.copies(j):
            copy.start()

    def finish(self, j):
        for copy in self.copies(j):
            copy.wait_recv()
        count = len(self.lands[j].shape)
        total = 1
        shape = tuple(reversed(self.radices[j:]))
        for s in shape:
            total *= s
        for flat in range(total):
            at, left = [], flat
            for s in reversed(shape):
                at.insert(0, left % s)
                left //= s
            at = tuple(at)
            if j == 0:
                value = self.read(flat, self.mp)
                lands = [self.lands[0][k, flat] for k in range(self.mp_size - 1)]
            else:
                digit = self.place[j - 1][0]
                value = self.sums[j - 1][at + (digit,)].astype(F32)
                lands = [self.lands[j][(k,) + at] for k in range(self.radices[j - 1] - 1)]
            for land in lands:
                value = value + land.astype(F32)
            if j < len(self.radices):
                self.sums[j][at] = value.astype(BF16)
            else:
                self.final[...] = value

    def drain(self):
        for j in range(len(self.radices) + 1):
            for copy in self.copies(j):
                copy.wait_send()


def block_kernel(n, mp_size, kv_radices, conv_radices, last_radices, *refs):
    (
        tsteps,
        levels,
        lengths,
        clean,
        noise,
        lowres,
        aug_noise,
        text,
        kv_weight,
        w_stem,
        w_time,
        conv_one,
        conv_two,
        w_query,
        w_output,
        w_head,
        one_out,
        two_out,
        kv_out,
        stat_out,
        emb_ref,
        kv_ref,
        cot_ref,
        kt_ref,
        kd_ref,
        vd_ref,
        vt_ref,
        wq_t,
        wo_t,
        wt_two,
        wh_ref,
        stem_lhs,
        noise_ref,
        norms,
        h_ref,
        xs_ref,
        a_one,
        a_two,
        gx_ref,
        c_ref,
        hm_ref,
        go_ref,
        dn_ref,
        g_one,
        acc_w,
        acc_k,
        acc_v,
        grad_one,
        grad_two,
        kv_land,
        kv_send,
        kv_recv,
        stat_ref,
        stat_land,
        stat_send,
        stat_recv,
        kv_blocks,
        one_blocks,
        two_blocks,
    ) = refs[:59]
    rest = refs[59:]
    sizes = [2 * len(r) + 3 for r in (kv_radices, last_radices, conv_radices)]
    kv_refs = rest[: sizes[0]]
    one_refs = rest[sizes[0] : sizes[0] + sizes[1]]
    two_refs = rest[sizes[0] + sizes[1] :]

    images, tokens, features = text.shape
    pixels = clean.shape[2]
    channels, width = w_query.shape
    span = TAPS * channels
    heads = w_head.shape[0]
    half = kv_weight.shape[0]
    dp_size = n // mp_size
    big = 1024
    mid = 1024
    count = float(pixels)
    my_dp, my_mp = lax.axis_index("dp"), lax.axis_index("mp")
    me = my_dp * mp_size + my_mp

    def place(t):
        return (lax.div(t, mp_size), lax.rem(t, mp_size))

    def over_peers(step):
        lax.fori_loop(0, n - 1, lambda k, c: (step(k), c)[1], 0)

    def target(k):
        return lax.rem(me + k + 1, n)

    barrier = pltpu.get_barrier_semaphore()
    over_peers(
        lambda k: pl.semaphore_signal(
            barrier, inc=1, device_id=place(target(k)), device_id_type=pl.DeviceIdType.MESH
        )
    )

    def chunks(size, body, init=0):
        return lax.fori_loop(0, pixels // size, lambda i, c: body(pl.multiple_of(i * size, size), c), init)

    zero8 = jnp.zeros((8, channels), F32)

    wq_t[...] = w_query[...].astype(F32).T.astype(BF16)
    wo_t[...] = w_output[...].astype(F32).T.astype(BF16)
    for dy in range(TAPS):
        for dx in range(TAPS):
            src = (TAPS * (TAPS - 1 - dy) + (TAPS - 1 - dx)) * channels
            dst = (TAPS * dy + dx) * channels
            wt_two[dst : dst + channels, :] = conv_two[src : src + channels, :].astype(F32).T.astype(BF16)
    wh_ref[...] = jnp.zeros_like(wh_ref)
    wh_ref[0:heads, :] = w_head[...].astype(F32)
    wh_ref[8 : 8 + heads, :] = w_head[...].astype(F32)
    wh = wh_ref[...].astype(BF16)
    stem_lhs[...] = jnp.zeros_like(stem_lhs)
    noise_ref[...] = jnp.zeros_like(noise_ref)
    stem_lhs[0, 0 : w_stem.shape[0], 0:channels] = w_stem[...]
    s1, s2, s3 = split3(stem_lhs[0, :, 0:channels])
    stem_w = jnp.concatenate([s1, s2, s1, s2, s3, s1], axis=0).astype(BF16)
    edge = jnp.zeros((S, span), BF16)
    for i in range(images):
        for ref in (a_one, a_two, gx_ref):
            ref[i, 0:S, :] = edge
            ref[i, S + pixels :, :] = edge
        t = jnp.full((8, 128), tsteps[i].astype(F32), F32)
        a = jnp.full((8, 128), levels[i].astype(F32), F32)
        signal, aug_signal = level_of(t), level_of(a)
        k1, k2 = jnp.sqrt(signal)[0:1, 0:1], jnp.sqrt(1.0 - signal)[0:1, 0:1]
        k3, k4 = jnp.sqrt(aug_signal)[0:1, 0:1], jnp.sqrt(1.0 - aug_signal)[0:1, 0:1]
        for k in range(heads):
            row = noise[k, i : i + 1, :]
            noise_ref[i, k : k + 1, :] = row
            stem_lhs[i, k : k + 1, :] = k1 * clean[k, i : i + 1, :] + k2 * row
            stem_lhs[i, heads + k : heads + k + 1, :] = k3 * lowres[k, i : i + 1, :] + k4 * aug_noise[k, i : i + 1, :]
    g_one[0:S, :] = edge[:, :channels]
    g_one[S + pixels :, :] = edge[:, :channels]
    grad_one[...] = jnp.zeros_like(grad_one)
    grad_two[...] = jnp.zeros_like(grad_two)

    lane = lax.broadcasted_iota(jnp.int32, (8, 4 * FREQS), 1)
    row = lax.broadcasted_iota(jnp.int32, (8, 4 * FREQS), 0)
    base = jnp.zeros((8, 4 * FREQS), F32)
    for i in range(images):
        both = jnp.where(lane < 2 * FREQS, tsteps[i].astype(F32), levels[i].astype(F32))
        base = jnp.where(row == i, both, base)
    freqs = jnp.exp(-math.log(10000.0) * (lane % FREQS).astype(F32) / FREQS)
    angles = base * freqs
    feature = jnp.where((lane // FREQS) % 2 == 0, jnp.sin(angles), jnp.cos(angles))
    emb = jnp.dot(feature, w_time[...], precision=lax.Precision.HIGHEST, preferred_element_type=F32)
    emb = emb * sigmoid(emb)
    for i in range(images):
        emb_ref[i] = jnp.broadcast_to(emb[i : i + 1], emb.shape)

    pl.semaphore_wait(barrier, n - 1)

    def kv_copy(k):
        return pltpu.make_async_remote_copy(
            src_ref=kv_weight,
            dst_ref=kv_land.at[k],
            send_sem=kv_send.at[k],
            recv_sem=kv_recv.at[k],
            device_id=(my_dp, lax.rem(my_mp + k + 1, mp_size)),
            device_id_type=pl.DeviceIdType.MESH,
        )

    for k in range(mp_size - 1):
        kv_copy(k).start()

    def shifted(dst, r0, size):
        x = lax.broadcasted_iota(jnp.int32, (size, channels), 0) % S
        window = xs_ref.at[pl.ds(r0, size + 16), :]
        left = window[7 : 7 + size, :]
        here = window[8 : 8 + size, :]
        right = window[9 : 9 + size, :]
        rows = pl.ds(r0 + S, size)
        dst[rows, 0:channels] = jnp.where(x == 0, 0.0, left).astype(BF16)
        dst[rows, channels : 2 * channels] = here.astype(BF16)
        dst[rows, 2 * channels : span] = jnp.where(x == S - 1, 0.0, right).astype(BF16)

    def convolve(src, weight, r0, size):
        total = None
        for dy in range(TAPS):
            part = dot(src[pl.ds(r0 + dy * S, size), :], weight[dy * span : (dy + 1) * span, :])
            total = part if total is None else total + part
        return total

    def weight_grad(src, g_src, lane0, grad):
        acc_w[...] = jnp.zeros_like(acc_w)

        def body(r0, carry):
            g = jnp.concatenate(
                [g_src[pl.ds(r0 + (2 - dy) * S, big), lane0 : lane0 + channels] for dy in range(TAPS)], axis=1
            )
            acc_w[...] += dot_lhs_t(src[pl.ds(r0 + S, big), :], g)
            return carry

        chunks(big, body)
        for dy in range(TAPS):
            part = acc_w[:, dy * channels : (dy + 1) * channels]
            grad[dy * span : (dy + 1) * span, :] += part.astype(BF16).astype(F32)

    def variance(ref, mean):
        def body(r0, acc):
            d = ref[pl.ds(r0, big), :] - mean
            return acc + fold(d * d)

        return lax.rsqrt(group_mean(chunks(big, body, zero8), count) + EPS)

    def keep_row(i, k, value):
        norms[i, k] = jnp.broadcast_to(value, (8, channels))

    def row_of(i, k):
        return norms[i, k, 0:1, :]

    def gain_bias(i):
        return 1.0 + emb_ref[i, 0:1, 0:channels], emb_ref[i, 0:1, channels : 2 * channels]

    def forward(i, carry):
        def stem(r0, acc):
            x1, x2, x3 = split3(stem_lhs[i, :, pl.ds(r0, big)])
            x = jnp.concatenate([x1, x1, x2, x2, x1, x3], axis=0).astype(BF16)
            h = dot_lhs_t(x, stem_w)
            h_ref[pl.ds(r0, big), :] = h
            return acc + fold(h)

        m1 = group_mean(chunks(big, stem, zero8), count)
        r1 = variance(h_ref, m1)

        def act_one(r0, c):
            x = (h_ref[pl.ds(r0, big), :] - m1) * r1
            xs_ref[pl.ds(r0 + 8, big), :] = x * sigmoid(x)
            return c

        one, two, conv, mid_map = a_one.at[i], a_two.at[i], c_ref.at[i], hm_ref.at[i]
        chunks(big, act_one)
        chunks(big, lambda r0, c: (shifted(one, r0, big), c)[1])

        def conv1(r0, acc):
            c = convolve(one, conv_one, r0, big)
            conv[pl.ds(r0, big), :] = c
            return acc + fold(c)

        m2 = group_mean(chunks(big, conv1, zero8), count)
        r2 = variance(conv, m2)
        gain, bias = gain_bias(i)

        def act_two(r0, c):
            z = (conv[pl.ds(r0, big), :] - m2) * r2 * gain + bias
            xs_ref[pl.ds(r0 + 8, big), :] = z * sigmoid(z)
            return c

        chunks(big, act_two)
        chunks(big, lambda r0, c: (shifted(two, r0, big), c)[1])

        def conv2(r0, acc):
            h = h_ref[pl.ds(r0, big), :] + convolve(two, conv_two, r0, big)
            mid_map[pl.ds(r0, big), :] = h
            return acc + fold(h)

        m3 = group_mean(chunks(big, conv2, zero8), count)
        r3 = variance(mid_map, m3)
        for k, value in enumerate((m2, r2, m3, r3)):
            keep_row(i, k, value)
        return carry

    lax.fori_loop(0, images, forward, 0)

    def features_of(m):
        cols = pl.ds(pl.multiple_of(m * half, half), half)
        return text[:, :, cols].reshape(images * tokens, half)

    kv = dot(features_of(my_mp), kv_weight[...])
    for k in range(mp_size - 1):
        kv_copy(k).wait_recv()
        kv += dot(features_of(lax.rem(my_mp + mp_size - k - 1, mp_size)), kv_land[k])
    kv_ref[...] = kv.astype(BF16).reshape(images, tokens, 2 * width)

    lane_w = lax.broadcasted_iota(jnp.int32, (tokens, width), 1)

    def attend(i, square):
        m3, r3 = row_of(i, 2), row_of(i, 3)
        keys = kv_ref[i, :, 0:width].astype(F32)
        values = kv_ref[i, :, width : 2 * width].astype(F32)
        for h in range(HEADS):
            mine = (lane_w // HEAD_DIM) == h
            k_h = jnp.where(mine, keys, 0.0)
            v_h = jnp.where(mine, values, 0.0)
            rows = slice(h * tokens, (h + 1) * tokens)
            kt_ref[:, rows] = k_h.T.astype(BF16)
            kd_ref[rows, :] = k_h.astype(BF16)
            vd_ref[rows, :] = v_h.astype(BF16)
            vt_ref[:, rows] = v_h.T.astype(BF16)
        acc_k[...] = jnp.zeros_like(acc_k)
        acc_v[...] = jnp.zeros_like(acc_v)
        length = lengths[i]
        scale = HEAD_DIM**-0.5
        mid_map = hm_ref.at[i]

        def attention(r0, carry):
            s1, s2, sq = carry
            rows = pl.ds(r0, mid)
            hm = mid_map[rows, :]
            xh = (hm - m3) * r3
            q = (dot(xh.astype(BF16), w_query[...]) * scale).astype(BF16)
            scores = dot(q, kt_ref[...])
            keep = lax.broadcasted_iota(jnp.int32, (mid, tokens), 1) < length
            probs = []
            for h in range(HEADS):
                s = jnp.where(keep, scores[:, h * tokens : (h + 1) * tokens], -1e30)
                w = jnp.exp(s - jnp.max(s, axis=1, keepdims=True))
                probs.append(w * (1.0 / jnp.sum(w, axis=1, keepdims=True)))
            pb = jnp.concatenate([p.astype(BF16) for p in probs], axis=1)
            attended = dot(pb, vd_ref[...]).astype(BF16)
            hob = (hm + dot(attended, w_output[...])).astype(BF16)
            error = dot_rhs_t(wh[0:8], hob) - noise_ref[i, :, rows]
            sq = sq + error * error
            e2 = error * 2.0
            high = e2.astype(BF16).astype(F32)
            e2 = jnp.concatenate([high, e2 - high], axis=0).astype(BF16)
            g = dot_lhs_t(e2, wh).astype(BF16)
            go_ref[rows, :] = g
            d_att = dot(g, wo_t[...]).astype(BF16)
            d_probs = dot(d_att, vt_ref[...]).astype(BF16).astype(F32)
            acc_v[...] += dot_lhs_t(pb, d_att)
            d_scores = []
            for h in range(HEADS):
                t = d_probs[:, h * tokens : (h + 1) * tokens] * probs[h]
                d_scores.append((t - probs[h] * jnp.sum(t, axis=1, keepdims=True)).astype(BF16))
            ds = jnp.concatenate(d_scores, axis=1)
            acc_k[...] += dot_lhs_t(ds, q)
            d_q = dot(ds, kd_ref[...]).astype(BF16)
            dn = (dot(d_q, wq_t[...]) * scale).astype(BF16)
            dn_ref[rows, :] = dn
            dx = dn.astype(F32)
            return s1 + fold(dx), s2 + fold(dx * xh), sq

        s1, s2, square = chunks(mid, attention, (zero8, zero8, square))
        n1, n2 = group_mean(s1, count), group_mean(s2, count)
        first = lane_w < HEAD_DIM
        cot_ref[i, :, 0:width] = jnp.where(first, acc_k[0:tokens, :], acc_k[tokens:, :]).astype(BF16)
        cot_ref[i, :, width : 2 * width] = jnp.where(first, acc_v[0:tokens, :], acc_v[tokens:, :]).astype(BF16)

        def d_mid(r0, c):
            rows = pl.ds(r0, big)
            xh = (mid_map[rows, :] - m3) * r3
            d = go_ref[rows, :].astype(F32) + r3 * (dn_ref[rows, :].astype(F32) - n1 - xh * n2)
            xs_ref[pl.ds(r0 + 8, big), :] = d
            return c

        chunks(big, d_mid)
        gx = gx_ref.at[i]
        chunks(big, lambda r0, c: (shifted(gx, r0, big), c)[1])
        return square

    square = lax.fori_loop(0, images, attend, jnp.zeros((8, mid), F32))

    cot = cot_ref[...].reshape(images * tokens, 2 * width)
    own = kv_blocks.shape[1]

    def project(j, c):
        cols = pl.ds(pl.multiple_of(j * big, big), big)
        value = dot_lhs_t(cot, text[:, :, cols].reshape(images * tokens, big)).astype(BF16)
        kv_blocks[:, :, cols] = value.reshape(dp_size, own, big)
        return c

    lax.fori_loop(0, features // big, project, 0)

    def kv_half(m):
        return pl.ds(pl.multiple_of(m * half, half), half)

    kv_sum = Scatter(
        lambda m: kv_blocks.at[:, :, kv_half(m)],
        lambda d, m: kv_blocks[d, :, kv_half(m)].astype(F32),
        kv_out,
        kv_radices,
        kv_refs,
        dp_size,
        mp_size,
    )

    def conv_sum(blocks, out, radices, refs):
        return Scatter(
            lambda m: blocks.at[m],
            lambda d, m: blocks[m, d].astype(F32),
            out,
            radices,
            refs,
            dp_size,
            mp_size,
        )

    one_sum = conv_sum(one_blocks, one_out, last_radices, one_refs)
    two_sum = conv_sum(two_blocks, two_out, conv_radices, two_refs)

    def cut(grad, blocks):
        rows = blocks.shape[2]
        for d in range(n):
            blocks[d % mp_size, d // mp_size] = grad[d * rows : (d + 1) * rows, :].astype(BF16)

    def second(i):
        weight_grad(a_two.at[i], gx_ref.at[i], channels, grad_two)

    def back(i):
        m2, r2 = row_of(i, 0), row_of(i, 1)
        gain, bias = gain_bias(i)
        gx, conv = gx_ref.at[i], c_ref.at[i]

        def d_act(r0, carry):
            s1, s2 = carry
            rows = pl.ds(r0, big)
            d = convolve(gx, wt_two, r0, big).astype(BF16).astype(F32)
            xh = (conv[rows, :] - m2) * r2
            z = xh * gain + bias
            sg = sigmoid(z)
            d = d * (sg * (1.0 + z * (1.0 - sg))) * gain
            h_ref[rows, :] = d
            return s1 + fold(d), s2 + fold(d * xh)

        s1, s2 = chunks(big, d_act, (zero8, zero8))
        n3, n4 = group_mean(s1, count), group_mean(s2, count)

        def d_conv(r0, c):
            rows = pl.ds(r0, big)
            xh = (conv[rows, :] - m2) * r2
            d = r2 * (h_ref[rows, :] - n3 - xh * n4)
            g_one[pl.ds(r0 + S, big), :] = d.astype(BF16)
            return c

        chunks(big, d_conv)

    def first(i):
        weight_grad(a_one.at[i], g_one, 0, grad_one)

    def steps_of(scatter):
        last = len(scatter.radices)
        for j in range(last + 1):
            if j == 0:
                scatter.start(0)
            else:
                scatter.finish(j - 1)
                scatter.start(j)
            yield
        scatter.finish(last)
        yield

    def lanes_total(x):
        return jnp.sum(jnp.sum(x, axis=0, keepdims=True), axis=1, keepdims=True)

    kv_steps = steps_of(kv_sum)
    next(kv_steps)
    for i in range(images):
        second(i)
    cut(grad_two, two_blocks)
    two_steps = steps_of(two_sum)
    next(kv_steps, None)
    next(two_steps, None)
    for i in range(images):
        back(i)
        next(kv_steps, None)
        next(two_steps, None)
        first(i)
        if i + 1 < images:
            next(kv_steps, None)
            next(two_steps, None)
    cut(grad_one, one_blocks)
    one_steps = steps_of(one_sum)
    next(one_steps)
    for _ in kv_steps:
        pass
    for _ in two_steps:
        pass
    for _ in one_steps:
        pass

    lane1 = lax.broadcasted_iota(jnp.int32, (1, 128), 1)
    parts = (
        lanes_total(one_out[...] * one_out[...]),
        lanes_total(two_out[...] * two_out[...]),
        lanes_total(kv_out[...] * kv_out[...]),
        lanes_total(square),
    )
    stat = jnp.zeros((1, 128), F32)
    for k, part in enumerate(parts):
        stat = jnp.where(lane1 == k, part, stat)
    stat_ref[...] = stat

    def stat_copy(k, slot):
        return pltpu.make_async_remote_copy(
            src_ref=stat_ref,
            dst_ref=stat_land.at[slot],
            send_sem=stat_send.at[k],
            recv_sem=stat_recv.at[k],
            device_id=place(target(k)),
            device_id_type=pl.DeviceIdType.MESH,
        )

    over_peers(lambda k: stat_copy(k, me).start())
    stat_land[me] = stat
    over_peers(lambda k: stat_copy(k, lax.rem(me + n - k - 1, n)).wait_recv())
    stat_out[...] = jnp.sum(stat_land[...], axis=0)
    over_peers(lambda k: stat_copy(k, me).wait_send())
    for k in range(mp_size - 1):
        kv_copy(k).wait_send()
    for scatter in (kv_sum, two_sum, one_sum):
        scatter.drain()


def scale_kernel(conv_count, kv_count, loss_count, one, two, kv, stats, one_out, two_out, kv_out, loss_out):
    row = stats[...]
    one_out[...] = one[...] * lax.rsqrt(row[:, 0:1] / conv_count + 1e-06)
    two_out[...] = two[...] * lax.rsqrt(row[:, 1:2] / conv_count + 1e-06)
    kv_out[...] = kv[...] * lax.rsqrt(row[:, 2:3] / kv_count + 1e-06)
    loss_out[...] = row[:, 3:4] / loss_count


def local(
    clean,
    noise,
    lowres,
    aug_noise,
    timesteps,
    aug_levels,
    lengths,
    text,
    w_stem,
    w_time,
    conv_one,
    conv_two,
    kv_weight,
    w_query,
    w_output,
    w_head,
):
    dp_size = lax.axis_size("dp")
    mp_size = lax.axis_size("mp")
    n = dp_size * mp_size
    images, tokens, features = text.shape
    pixels = clean.shape[2]
    channels, width = w_query.shape
    span = TAPS * channels
    half = kv_weight.shape[0]
    own = 2 * width // dp_size
    rows = conv_one.shape[0] // n
    kv_radices = conv_radices = last_radices = radices_of(dp_size)
    turn = lambda x: jnp.transpose(x, (1, 0, 2))
    arrays = (
        turn(clean),
        turn(noise),
        turn(lowres),
        turn(aug_noise),
        text,
        kv_weight,
        w_stem,
        w_time,
        conv_one,
        conv_two,
        w_query,
        w_output,
        w_head,
    )
    vmem = pl.BlockSpec(memory_space=pltpu.VMEM)
    smem = pl.BlockSpec(memory_space=pltpu.SMEM)
    v = pltpu.VMEM
    dma = pltpu.SemaphoreType.DMA
    padded = pixels + 2 * S
    conv_block = (rows, channels)
    one, two, kv, stats = pl.pallas_call(
        functools.partial(block_kernel, n, mp_size, kv_radices, conv_radices, last_radices),
        out_shape=(
            jax.ShapeDtypeStruct(conv_block, F32),
            jax.ShapeDtypeStruct(conv_block, F32),
            jax.ShapeDtypeStruct((own, half), F32),
            jax.ShapeDtypeStruct((1, 128), F32),
        ),
        in_specs=[smem] * 3 + [vmem] * len(arrays),
        out_specs=(vmem,) * 4,
        scratch_shapes=[
            v((images, 8, 2 * channels), F32),
            v((images, tokens, 2 * width), BF16),
            v((images, tokens, 2 * width), BF16),
            v((width, HEADS * tokens), BF16),
            v((HEADS * tokens, width), BF16),
            v((HEADS * tokens, width), BF16),
            v((width, HEADS * tokens), BF16),
            v((width, channels), BF16),
            v((channels, width), BF16),
            v((TAPS * span, channels), BF16),
            v((16, channels), F32),
            v((images, 8, pixels), F32),
            v((images, 8, pixels), F32),
            v((images, 4, 8, channels), F32),
            v((pixels, channels), F32),
            v((pixels + 16, channels), F32),
            v((images, padded, span), BF16),
            v((images, padded, span), BF16),
            v((images, padded, span), BF16),
            v((images, pixels, channels), F32),
            v((images, pixels, channels), F32),
            v((pixels, channels), BF16),
            v((pixels, channels), BF16),
            v((padded, channels), BF16),
            v((span, span), F32),
            v((HEADS * tokens, width), F32),
            v((HEADS * tokens, width), F32),
            v(conv_one.shape, F32),
            v(conv_one.shape, F32),
            v((mp_size - 1,) + kv_weight.shape, BF16),
            dma((mp_size - 1,)),
            dma((mp_size - 1,)),
            v((1, 128), F32),
            v((n, 1, 128), F32),
            dma((n - 1,)),
            dma((n - 1,)),
            v((dp_size, own, features), BF16),
            v((mp_size, dp_size) + conv_block, BF16),
            v((mp_size, dp_size) + conv_block, BF16),
        ]
        + scratch_of((own, half), kv_radices, dp_size, mp_size)
        + scratch_of(conv_block, last_radices, dp_size, mp_size)
        + scratch_of(conv_block, conv_radices, dp_size, mp_size),
        compiler_params=pltpu.CompilerParams(
            collective_id=0, has_side_effects=True, vmem_limit_bytes=62 * 1024 * 1024
        ),
    )(timesteps, aug_levels, lengths, *arrays)
    conv_count = conv_one.shape[0] * conv_one.shape[1]
    kv_count = half * mp_size * 2 * width
    loss_count = images * n * clean.shape[1] * pixels
    one, two, kv, loss = pl.pallas_call(
        functools.partial(scale_kernel, conv_count, kv_count, loss_count),
        out_shape=(
            jax.ShapeDtypeStruct(conv_block, F32),
            jax.ShapeDtypeStruct(conv_block, F32),
            jax.ShapeDtypeStruct((own, half), F32),
            jax.ShapeDtypeStruct((1, 1), F32),
        ),
        in_specs=[vmem] * 4,
        out_specs=(vmem,) * 4,
    )(one, two, kv, stats)
    return (one, two, kv.T, loss.reshape(()))


def solution(mesh):
    return jax.shard_map(
        local,
        mesh=mesh,
        in_specs=(
            P(("dp", "mp"), None, None),
            P(("dp", "mp"), None, None),
            P(("dp", "mp"), None, None),
            P(("dp", "mp"), None, None),
            P(("dp", "mp")),
            P(("dp", "mp")),
            P(("dp", "mp")),
            P(("dp", "mp"), None, None),
            P(),
            P(),
            P(),
            P(),
            P("mp", None),
            P(),
            P(),
            P(),
        ),
        out_specs=(P(("dp", "mp"), None), P(("dp", "mp"), None), P("mp", "dp"), P()),
        check_vma=False,
    )
```

```python
import functools
import math

import jax
import jax.numpy as jnp
from jax import lax
from jax.experimental import pallas as pl
from jax.experimental.pallas import tpu as pltpu
from jax.sharding import PartitionSpec as P

S = 64
GROUPS = 32
HEADS = 2
HEAD_DIM = 64
FREQS = 64
STEPS = 1000
F32 = jnp.float32
BF16 = jnp.bfloat16
EPS = 1e-05
TAPS = 3


def level_of(index):
    ratio = (index / STEPS + 0.008) / 1.008
    cosine = jnp.cos(ratio * (math.pi / 2.0))
    return cosine * cosine


def dot(a, b):
    return jnp.dot(a, b, preferred_element_type=F32)


def dot_lhs_t(a, b):
    return lax.dot_general(a, b, (((0,), (0,)), ((), ())), preferred_element_type=F32)


def dot_rhs_t(a, b):
    return lax.dot_general(a, b, (((1,), (1,)), ((), ())), preferred_element_type=F32)


def fold(values):
    rows, lanes = values.shape
    return jnp.sum(values.reshape(rows // 8, 8, lanes), axis=0)


def group_avg(row):
    channels = row.shape[1]
    total = jnp.broadcast_to(row, (8, channels))
    lane = lax.broadcasted_iota(jnp.int32, total.shape, 1)
    members = channels // GROUPS
    step = 1
    while step < members:
        up = pltpu.roll(total, channels - step, 1)
        down = pltpu.roll(total, step, 1)
        total = total + jnp.where((lane // step) % 2 == 0, up, down)
        step *= 2
    return total[0:1] / members


def group_mean(acc, count):
    return group_avg(jnp.sum(acc, axis=0, keepdims=True) / count)


def moments(values, first, carry):
    center, total, square = carry
    part = fold(values)
    here = jnp.sum(part, axis=0, keepdims=True) / values.shape[0]
    center = jnp.where(first, here, center)
    d = values - center
    return center, total + part, square + fold(d * d)


def norm_of(carry, count):
    center, total, square = carry
    mean = jnp.sum(total, axis=0, keepdims=True) / count
    within = jnp.sum(square, axis=0, keepdims=True) / count - (mean - center) * (mean - center)
    average = group_avg(mean)
    spread = group_avg(within + (mean - average) * (mean - average))
    return average, lax.rsqrt(spread + EPS)


def sigmoid(x):
    return 1.0 / (1.0 + jnp.exp(-x))


def split3(x):
    one = x.astype(BF16).astype(F32)
    two = (x - one).astype(BF16).astype(F32)
    three = (x - one - two).astype(BF16).astype(F32)
    return one, two, three


def radices_of(size):
    parts = []
    for step in (2, 2):
        if size % step == 0 and size > 1:
            parts.append(step)
            size //= step
    while size > 1:
        step = next((s for s in (4, 2, 3, 5, 7) if size % s == 0), size)
        parts.append(step)
        size //= step
    return tuple(parts)


def order_of(radices, turned=False):
    out, stride = [], 1
    for radix in radices:
        out.append((radix, stride))
        stride *= radix
    if turned and len(out) > 1:
        out[0], out[1] = out[1], out[0]
    return tuple(out)


def blocks_of(shape, radices):
    return [tuple(reversed(radices[j:])) + tuple(shape) for j in range(len(radices))]


def lands_of(shape, radices, dp_size, mp_size):
    lands = [(mp_size - 1, dp_size) + tuple(shape)]
    for j, radix in enumerate(radices):
        lands.append((radix - 1,) + tuple(reversed(radices[j + 1 :])) + tuple(shape))
    return lands


def scratch_of(shape, order, dp_size, mp_size):
    radices = [r for r, _ in order]
    copies = mp_size - 1 + sum(r - 1 for r in radices)
    return (
        [pltpu.VMEM(s, BF16) for s in blocks_of(shape, radices)]
        + [pltpu.VMEM(s, BF16) for s in lands_of(shape, radices, dp_size, mp_size)]
        + [pltpu.SemaphoreType.DMA((copies,)), pltpu.SemaphoreType.DMA((copies,))]
    )


class Scatter:
    def __init__(self, pick, read, final, order, refs, dp_size, mp_size):
        radices, strides = zip(*order)
        k = len(radices)
        self.pick, self.read, self.final, self.radices = pick, read, final, radices
        self.sums, self.lands = refs[:k], refs[k : 2 * k + 1]
        self.send, self.recv = refs[2 * k + 1 :]
        self.dp_size, self.mp_size = dp_size, mp_size
        self.dp, self.mp = lax.axis_index("dp"), lax.axis_index("mp")
        self.strides = strides
        self.place = [(lax.rem(lax.div(self.dp, t), r), t) for r, t in zip(radices, strides)]

    def copies(self, j):
        out = []
        if j == 0:
            for k in range(self.mp_size - 1):
                peer = lax.rem(self.mp + k + 1, self.mp_size)
                out.append((self.pick(peer), self.lands[0].at[k], k, (self.dp, peer)))
        else:
            radix = self.radices[j - 1]
            digit, stride = self.place[j - 1]
            first = self.mp_size - 1 + sum(r - 1 for r in self.radices[: j - 1])
            rest = len(self.radices) - j
            for k in range(radix - 1):
                there = lax.rem(digit + k + 1, radix)
                src = self.sums[j - 1].at[(slice(None),) * rest + (there,)]
                peer = self.dp + (there - digit) * stride
                out.append((src, self.lands[j].at[k], first + k, (peer, self.mp)))
        return [
            pltpu.make_async_remote_copy(
                src_ref=src,
                dst_ref=dst,
                send_sem=self.send.at[sem],
                recv_sem=self.recv.at[sem],
                device_id=peer,
                device_id_type=pl.DeviceIdType.MESH,
            )
            for src, dst, sem, peer in out
        ]

    def start(self, j):
        for copy in self.copies(j):
            copy.start()

    def finish(self, j):
        for copy in self.copies(j):
            copy.wait_recv()
        count = len(self.lands[j].shape)
        total = 1
        shape = tuple(reversed(self.radices[j:]))
        for s in shape:
            total *= s
        for flat in range(total):
            at, left = [], flat
            for s in reversed(shape):
                at.insert(0, left % s)
                left //= s
            at = tuple(at)
            if j == 0:
                block = sum(a * t for a, t in zip(at, reversed(self.strides)))
                value = self.read(block, self.mp)
                lands = [self.lands[0][k, block] for k in range(self.mp_size - 1)]
            else:
                digit = self.place[j - 1][0]
                value = self.sums[j - 1][at + (digit,)].astype(F32)
                lands = [self.lands[j][(k,) + at] for k in range(self.radices[j - 1] - 1)]
            for land in lands:
                value = value + land.astype(F32)
            if j < len(self.radices):
                self.sums[j][at] = value.astype(BF16)
            else:
                self.final(value)

    def drain(self):
        for j in range(len(self.radices) + 1):
            for copy in self.copies(j):
                copy.wait_send()


def block_kernel(n, mp_size, orders, *refs):
    (
        tsteps,
        levels,
        lengths,
        clean,
        noise,
        lowres,
        aug_noise,
        text_hbm,
        kv_weight,
        w_stem,
        w_time,
        conv_one,
        conv_two,
        w_query,
        w_output,
        w_head,
        one_out,
        two_out,
        kv_out,
        stat_out,
        emb_ref,
        kv_ref,
        cot_ref,
        kt_ref,
        kd_ref,
        vd_ref,
        vt_ref,
        wq_t,
        wo_t,
        tap_one,
        tap_two,
        tap_back,
        wh_ref,
        stem_lhs,
        noise_ref,
        norms,
        h_ref,
        xs_ref,
        a_one,
        a_two,
        gx_ref,
        c_ref,
        hm_ref,
        go_ref,
        dn_ref,
        g_one,
        acc_w,
        acc_k,
        acc_v,
        grad_one,
        grad_two,
        text,
        kv_own,
        load_sem,
        kv_land,
        kv_send,
        kv_recv,
        stat_ref,
        stat_land,
        stat_send,
        stat_recv,
        kv_blocks,
        one_blocks,
        two_blocks,
    ) = refs[:64]
    rest = list(refs[64:])
    groups = []
    for order in orders:
        size = 2 * len(order) + 3
        groups.append(rest[:size])
        rest = rest[size:]

    images, tokens, features = text.shape
    pixels = clean.shape[2]
    channels, width = w_query.shape
    span = TAPS * channels
    heads = w_head.shape[0]
    half = kv_weight.shape[0]
    dp_size = n // mp_size
    big = 2048
    mid = 2048
    count = float(pixels)
    lines = pixels // S
    my_dp, my_mp = lax.axis_index("dp"), lax.axis_index("mp")
    me = my_dp * mp_size + my_mp

    def place(t):
        return (lax.div(t, mp_size), lax.rem(t, mp_size))

    def over_peers(step):
        lax.fori_loop(0, n - 1, lambda k, c: (step(k), c)[1], 0)

    def target(k):
        return lax.rem(me + k + 1, n)

    text_load = pltpu.make_async_copy(text_hbm, text, load_sem.at[0])
    own_load = pltpu.make_async_copy(kv_weight, kv_own, load_sem.at[1])
    text_load.start()
    own_load.start()
    barrier = pltpu.get_barrier_semaphore()
    over_peers(
        lambda k: pl.semaphore_signal(
            barrier, inc=1, device_id=place(target(k)), device_id_type=pl.DeviceIdType.MESH
        )
    )

    def chunks(size, body, init=0):
        return lax.fori_loop(0, pixels // size, lambda i, c: body(pl.multiple_of(i * size, size), c), init)

    zero8 = jnp.zeros((8, channels), F32)

    wq_t[...] = w_query[...].astype(F32).T.astype(BF16)
    wo_t[...] = w_output[...].astype(F32).T.astype(BF16)
    none = jnp.zeros((span, channels), BF16)
    for taps, weight in ((tap_one, conv_one), (tap_two, conv_two)):
        for parity in range(2):
            lanes = slice(parity * channels, (parity + 1) * channels)
            for j in range(TAPS + 1):
                dy = j - parity
                piece = weight[dy * span : (dy + 1) * span, :] if 0 <= dy < TAPS else none
                taps[j * span : (j + 1) * span, lanes] = piece
    for dy in range(TAPS):
        for dx in range(TAPS):
            src = (TAPS * (TAPS - 1 - dy) + (TAPS - 1 - dx)) * channels
            piece = conv_two[src : src + channels, :].astype(F32).T.astype(BF16)
            for parity in range(2):
                dst = (dy + parity) * span + dx * channels
                tap_back[dst : dst + channels, parity * channels : (parity + 1) * channels] = piece
    tap_back[0:span, channels : 2 * channels] = none
    tap_back[TAPS * span : (TAPS + 1) * span, 0:channels] = none
    wh_ref[...] = jnp.zeros_like(wh_ref)
    wh_ref[0:heads, :] = w_head[...].astype(F32)
    wh_ref[8 : 8 + heads, :] = w_head[...].astype(F32)
    wh = wh_ref[...].astype(BF16)
    stem_lhs[...] = jnp.zeros_like(stem_lhs)
    noise_ref[...] = jnp.zeros_like(noise_ref)
    stem_lhs[0, 0 : w_stem.shape[0], 0:channels] = w_stem[...]
    s1, s2, s3 = split3(stem_lhs[0, :, 0:channels])
    stem_w = jnp.concatenate([s1, s2, s1, s2, s3, s1], axis=0).astype(BF16)
    edge = jnp.zeros((S, span), BF16)
    for i in range(images):
        for ref in (a_one, a_two, gx_ref):
            ref[i, 0] = edge
            ref[i, lines + 1] = edge
        t = jnp.full((8, 128), tsteps[i].astype(F32), F32)
        a = jnp.full((8, 128), levels[i].astype(F32), F32)
        signal, aug_signal = level_of(t), level_of(a)
        k1, k2 = jnp.sqrt(signal)[0:1, 0:1], jnp.sqrt(1.0 - signal)[0:1, 0:1]
        k3, k4 = jnp.sqrt(aug_signal)[0:1, 0:1], jnp.sqrt(1.0 - aug_signal)[0:1, 0:1]
        for k in range(heads):
            row = noise[k, i : i + 1, :]
            noise_ref[i, k : k + 1, :] = row
            stem_lhs[i, k : k + 1, :] = k1 * clean[k, i : i + 1, :] + k2 * row
            stem_lhs[i, heads + k : heads + k + 1, :] = k3 * lowres[k, i : i + 1, :] + k4 * aug_noise[k, i : i + 1, :]
    g_one[0] = edge[:, :channels]
    g_one[lines + 1] = edge[:, :channels]
    grad_one[...] = jnp.zeros_like(grad_one)
    grad_two[...] = jnp.zeros_like(grad_two)

    lane = lax.broadcasted_iota(jnp.int32, (8, 4 * FREQS), 1)
    row = lax.broadcasted_iota(jnp.int32, (8, 4 * FREQS), 0)
    base = jnp.zeros((8, 4 * FREQS), F32)
    for i in range(images):
        both = jnp.where(lane < 2 * FREQS, tsteps[i].astype(F32), levels[i].astype(F32))
        base = jnp.where(row == i, both, base)
    freqs = jnp.exp(-math.log(10000.0) * (lane % FREQS).astype(F32) / FREQS)
    angles = base * freqs
    feature = jnp.where((lane // FREQS) % 2 == 0, jnp.sin(angles), jnp.cos(angles))
    emb = jnp.dot(feature, w_time[...], precision=lax.Precision.HIGHEST, preferred_element_type=F32)
    emb = emb * sigmoid(emb)
    for i in range(images):
        emb_ref[i] = jnp.broadcast_to(emb[i : i + 1], emb.shape)

    def kv_copy(k):
        return pltpu.make_async_remote_copy(
            src_ref=kv_weight,
            dst_ref=kv_land.at[k],
            send_sem=kv_send.at[k],
            recv_sem=kv_recv.at[k],
            device_id=(my_dp, lax.rem(my_mp + k + 1, mp_size)),
            device_id_type=pl.DeviceIdType.MESH,
        )

    def fetch():
        pl.semaphore_wait(barrier, n - 1)
        for k in range(mp_size - 1):
            kv_copy(k).start()

    def shifted(dst, r0, size):
        x = lax.broadcasted_iota(jnp.int32, (size, channels), 0) % S
        window = xs_ref.at[pl.ds(r0, size + 16), :]
        left = window[7 : 7 + size, :]
        here = window[8 : 8 + size, :]
        right = window[9 : 9 + size, :]
        rows = pl.ds(r0 // S + 1, size // S)
        shape = (size // S, S, channels)
        dst[rows, :, 0:channels] = jnp.where(x == 0, 0.0, left).astype(BF16).reshape(shape)
        dst[rows, :, channels : 2 * channels] = here.astype(BF16).reshape(shape)
        dst[rows, :, 2 * channels : span] = jnp.where(x == S - 1, 0.0, right).astype(BF16).reshape(shape)

    def convolve(src, taps, r0, size):
        y0 = r0 // S
        pairs = size // S // 2
        pieces = [
            jnp.concatenate([src[y0 + 2 * t + j] for t in range(pairs)], axis=0) for j in range(TAPS + 1)
        ]
        out = dot(jnp.concatenate(pieces, axis=1), taps[...])
        rows = []
        for t in range(pairs):
            for parity in range(2):
                rows.append(out[t * S : (t + 1) * S, parity * channels : (parity + 1) * channels])
        return jnp.concatenate(rows, axis=0)

    def weight_grad(src, g_src, lane0, grad):
        acc_w[...] = jnp.zeros_like(acc_w)

        def body(r0, carry):
            y0 = r0 // S
            g = jnp.concatenate(
                [
                    g_src[pl.ds(y0 + 2 - dy, big // S), :, lane0 : lane0 + channels].reshape(big, channels)
                    for dy in range(TAPS)
                ],
                axis=1,
            )
            acc_w[...] += dot_lhs_t(src[pl.ds(y0 + 1, big // S)].reshape(big, span), g)
            return carry

        chunks(big, body)
        for dy in range(TAPS):
            part = acc_w[:, dy * channels : (dy + 1) * channels]
            grad[dy * span : (dy + 1) * span, :] += part.astype(BF16).astype(F32)

    start_sums = (jnp.zeros((1, channels), F32), zero8, zero8)

    def keep_row(i, k, value):
        norms[i, k] = jnp.broadcast_to(value, (8, channels))

    def row_of(i, k):
        return norms[i, k, 0:1, :]

    def gain_bias(i):
        return 1.0 + emb_ref[i, 0:1, 0:channels], emb_ref[i, 0:1, channels : 2 * channels]

    def forward(i, carry):
        pl.when(i == images - 1)(fetch)

        def stem(r0, acc):
            x1, x2, x3 = split3(stem_lhs[i, :, pl.ds(r0, big)])
            x = jnp.concatenate([x1, x1, x2, x2, x1, x3], axis=0).astype(BF16)
            h = dot_lhs_t(x, stem_w)
            h_ref[pl.ds(r0, big), :] = h
            return moments(h, r0 == 0, acc)

        m1, r1 = norm_of(chunks(big, stem, start_sums), count)

        def act_one(r0, c):
            x = (h_ref[pl.ds(r0, big), :] - m1) * r1
            xs_ref[pl.ds(r0 + 8, big), :] = x * sigmoid(x)
            return c

        one, two, conv, mid_map = a_one.at[i], a_two.at[i], c_ref.at[i], hm_ref.at[i]
        chunks(big, act_one)
        chunks(big, lambda r0, c: (shifted(one, r0, big), c)[1])

        def conv1(r0, acc):
            c = convolve(one, tap_one, r0, big)
            conv[pl.ds(r0, big), :] = c
            return moments(c, r0 == 0, acc)

        m2, r2 = norm_of(chunks(big, conv1, start_sums), count)
        gain, bias = gain_bias(i)

        def act_two(r0, c):
            z = (conv[pl.ds(r0, big), :] - m2) * r2 * gain + bias
            xs_ref[pl.ds(r0 + 8, big), :] = z * sigmoid(z)
            return c

        chunks(big, act_two)
        chunks(big, lambda r0, c: (shifted(two, r0, big), c)[1])

        def conv2(r0, acc):
            h = h_ref[pl.ds(r0, big), :] + convolve(two, tap_two, r0, big)
            mid_map[pl.ds(r0, big), :] = h
            return moments(h, r0 == 0, acc)

        m3, r3 = norm_of(chunks(big, conv2, start_sums), count)
        for k, value in enumerate((m2, r2, m3, r3)):
            keep_row(i, k, value)
        return carry

    lax.fori_loop(0, images, forward, 0)

    def features_of(m):
        cols = pl.ds(pl.multiple_of(m * half, half), half)
        return text[:, :, cols].reshape(images * tokens, half)

    text_load.wait()
    own_load.wait()
    kv = dot(features_of(my_mp), kv_own[...])
    for k in range(mp_size - 1):
        kv_copy(k).wait_recv()
        kv += dot(features_of(lax.rem(my_mp + mp_size - k - 1, mp_size)), kv_land[k])
    kv_ref[...] = kv.astype(BF16).reshape(images, tokens, 2 * width)

    lane_w = lax.broadcasted_iota(jnp.int32, (tokens, width), 1)

    def attend(i, square):
        m3, r3 = row_of(i, 2), row_of(i, 3)
        keys = kv_ref[i, :, 0:width].astype(F32)
        values = kv_ref[i, :, width : 2 * width].astype(F32)
        for h in range(HEADS):
            mine = (lane_w // HEAD_DIM) == h
            k_h = jnp.where(mine, keys, 0.0)
            v_h = jnp.where(mine, values, 0.0)
            rows = slice(h * tokens, (h + 1) * tokens)
            kt_ref[:, rows] = k_h.T.astype(BF16)
            kd_ref[rows, :] = k_h.astype(BF16)
            vd_ref[rows, :] = v_h.astype(BF16)
            vt_ref[:, rows] = v_h.T.astype(BF16)
        acc_k[...] = jnp.zeros_like(acc_k)
        acc_v[...] = jnp.zeros_like(acc_v)
        length = lengths[i]
        scale = HEAD_DIM**-0.5
        mid_map = hm_ref.at[i]

        def attention(r0, carry):
            s1, s2, sq = carry
            rows = pl.ds(r0, mid)
            hm = mid_map[rows, :]
            xh = (hm - m3) * r3
            q = (dot(xh.astype(BF16), w_query[...]) * scale).astype(BF16)
            scores = dot(q, kt_ref[...])
            keep = lax.broadcasted_iota(jnp.int32, (mid, tokens), 1) < length
            probs = []
            for h in range(HEADS):
                s = jnp.where(keep, scores[:, h * tokens : (h + 1) * tokens], -1e30)
                w = jnp.exp(s - jnp.max(s, axis=1, keepdims=True))
                probs.append(w * (1.0 / jnp.sum(w, axis=1, keepdims=True)))
            pb = jnp.concatenate([p.astype(BF16) for p in probs], axis=1)
            attended = dot(pb, vd_ref[...]).astype(BF16)
            hob = (hm + dot(attended, w_output[...])).astype(BF16)
            error = dot_rhs_t(wh[0:8], hob) - noise_ref[i, :, rows]
            sq = sq + error * error
            e2 = error * 2.0
            high = e2.astype(BF16).astype(F32)
            e2 = jnp.concatenate([high, e2 - high], axis=0).astype(BF16)
            g = dot_lhs_t(e2, wh).astype(BF16)
            go_ref[rows, :] = g
            d_att = dot(g, wo_t[...]).astype(BF16)
            d_probs = dot(d_att, vt_ref[...]).astype(BF16).astype(F32)
            acc_v[...] += dot_lhs_t(pb, d_att)
            d_scores = []
            for h in range(HEADS):
                t = d_probs[:, h * tokens : (h + 1) * tokens] * probs[h]
                d_scores.append((t - probs[h] * jnp.sum(t, axis=1, keepdims=True)).astype(BF16))
            ds = jnp.concatenate(d_scores, axis=1)
            acc_k[...] += dot_lhs_t(ds, q)
            d_q = dot(ds, kd_ref[...]).astype(BF16)
            dn = (dot(d_q, wq_t[...]) * scale).astype(BF16)
            dn_ref[rows, :] = dn
            dx = dn.astype(F32)
            return s1 + fold(dx), s2 + fold(dx * xh), sq

        s1, s2, square = chunks(mid, attention, (zero8, zero8, square))
        n1, n2 = group_mean(s1, count), group_mean(s2, count)
        first = lane_w < HEAD_DIM
        cot_ref[i, :, 0:width] = jnp.where(first, acc_k[0:tokens, :], acc_k[tokens:, :]).astype(BF16)
        cot_ref[i, :, width : 2 * width] = jnp.where(first, acc_v[0:tokens, :], acc_v[tokens:, :]).astype(BF16)

        def d_mid(r0, c):
            rows = pl.ds(r0, big)
            xh = (mid_map[rows, :] - m3) * r3
            d = go_ref[rows, :].astype(F32) + r3 * (dn_ref[rows, :].astype(F32) - n1 - xh * n2)
            xs_ref[pl.ds(r0 + 8, big), :] = d
            return c

        chunks(big, d_mid)
        gx = gx_ref.at[i]
        chunks(big, lambda r0, c: (shifted(gx, r0, big), c)[1])
        return square

    square = lax.fori_loop(0, images, attend, jnp.zeros((8, mid), F32))

    cot = cot_ref[...].reshape(images * tokens, 2 * width)
    own = kv_blocks.shape[1]

    def project(j, c):
        cols = pl.ds(pl.multiple_of(j * big, big), big)
        value = dot_lhs_t(cot, text[:, :, cols].reshape(images * tokens, big)).astype(BF16)
        kv_blocks[:, :, cols] = value.reshape(dp_size, own, big)
        return c

    lax.fori_loop(0, features // big, project, 0)

    colors = len(orders) - 2
    lane_step = half // colors

    def kv_part(m, c):
        return pl.ds(pl.multiple_of(m * half + c * lane_step, lane_step), lane_step)

    def kv_sum(c):
        def final(value):
            kv_out[:, c * lane_step : (c + 1) * lane_step] = value

        return Scatter(
            lambda m: kv_blocks.at[:, :, kv_part(m, c)],
            lambda d, m: kv_blocks[d, :, kv_part(m, c)].astype(F32),
            final,
            orders[c],
            groups[c],
            dp_size,
            mp_size,
        )

    def conv_sum(blocks, out, k):
        def final(value):
            out[...] = value

        return Scatter(
            lambda m: blocks.at[m],
            lambda d, m: blocks[m, d].astype(F32),
            final,
            orders[k],
            groups[k],
            dp_size,
            mp_size,
        )

    kv_sums = [kv_sum(c) for c in range(colors)]
    two_sum = conv_sum(two_blocks, two_out, colors)
    one_sum = conv_sum(one_blocks, one_out, colors + 1)

    def cut(grad, blocks):
        rows = blocks.shape[2]
        for d in range(n):
            blocks[d % mp_size, d // mp_size] = grad[d * rows : (d + 1) * rows, :].astype(BF16)

    def second(i):
        weight_grad(a_two.at[i], gx_ref.at[i], channels, grad_two)

    def back(i, between):
        m2, r2 = row_of(i, 0), row_of(i, 1)
        gain, bias = gain_bias(i)
        gx, conv = gx_ref.at[i], c_ref.at[i]

        def d_act(r0, carry):
            s1, s2 = carry
            rows = pl.ds(r0, big)
            d = convolve(gx, tap_back, r0, big).astype(BF16).astype(F32)
            xh = (conv[rows, :] - m2) * r2
            z = xh * gain + bias
            sg = sigmoid(z)
            d = d * (sg * (1.0 + z * (1.0 - sg))) * gain
            h_ref[rows, :] = d
            return s1 + fold(d), s2 + fold(d * xh)

        s1, s2 = chunks(big, d_act, (zero8, zero8))
        n3, n4 = group_mean(s1, count), group_mean(s2, count)
        between()

        def d_conv(r0, c):
            rows = pl.ds(r0, big)
            xh = (conv[rows, :] - m2) * r2
            d = r2 * (h_ref[rows, :] - n3 - xh * n4)
            g_one[pl.ds(r0 // S + 1, big // S)] = d.astype(BF16).reshape(big // S, S, channels)
            return c

        chunks(big, d_conv)

    def first(i):
        weight_grad(a_one.at[i], g_one, 0, grad_one)

    def steps_of(scatter):
        group = scatter if isinstance(scatter, list) else [scatter]
        last = len(group[0].radices)
        for j in range(last + 2):
            for one in group:
                if j > 0:
                    one.finish(j - 1)
                if j <= last:
                    one.start(j)
            yield

    def lanes_total(x):
        return jnp.sum(jnp.sum(x, axis=0, keepdims=True), axis=1, keepdims=True)

    kv_steps = steps_of(kv_sums)
    two_steps = steps_of(two_sum)
    next(kv_steps)
    for i in range(images):
        second(i)
        if i == 0:
            next(kv_steps, None)
    cut(grad_two, two_blocks)
    next(two_steps)
    for i in range(images):
        back(i, lambda: (next(kv_steps, None), next(two_steps, None)))
        first(i)
        if i + 1 < images:
            next(kv_steps, None)
            next(two_steps, None)
    cut(grad_one, one_blocks)
    one_steps = steps_of(one_sum)
    next(one_steps)
    for _ in kv_steps:
        pass
    for _ in two_steps:
        pass
    for _ in one_steps:
        pass

    lane1 = lax.broadcasted_iota(jnp.int32, (1, 128), 1)
    parts = (
        lanes_total(one_out[...] * one_out[...]),
        lanes_total(two_out[...] * two_out[...]),
        lanes_total(kv_out[...] * kv_out[...]),
        lanes_total(square),
    )
    stat = jnp.zeros((1, 128), F32)
    for k, part in enumerate(parts):
        stat = jnp.where(lane1 == k, part, stat)
    stat_ref[...] = stat

    def stat_copy(k, slot):
        return pltpu.make_async_remote_copy(
            src_ref=stat_ref,
            dst_ref=stat_land.at[slot],
            send_sem=stat_send.at[k],
            recv_sem=stat_recv.at[k],
            device_id=place(target(k)),
            device_id_type=pl.DeviceIdType.MESH,
        )

    over_peers(lambda k: stat_copy(k, me).start())
    stat_land[me] = stat
    over_peers(lambda k: stat_copy(k, lax.rem(me + n - k - 1, n)).wait_recv())
    stat_out[...] = jnp.sum(stat_land[...], axis=0)
    over_peers(lambda k: stat_copy(k, me).wait_send())
    for k in range(mp_size - 1):
        kv_copy(k).wait_send()
    for scatter in (*kv_sums, two_sum, one_sum):
        scatter.drain()


def scale_kernel(conv_count, kv_count, loss_count, one, two, kv, stats, one_out, two_out, kv_out, loss_out):
    row = stats[...]
    one_out[...] = one[...] * lax.rsqrt(row[:, 0:1] / conv_count + 1e-06)
    two_out[...] = two[...] * lax.rsqrt(row[:, 1:2] / conv_count + 1e-06)
    kv_out[...] = kv[...] * lax.rsqrt(row[:, 2:3] / kv_count + 1e-06)
    loss_out[...] = row[:, 3:4] / loss_count


def local(
    clean,
    noise,
    lowres,
    aug_noise,
    timesteps,
    aug_levels,
    lengths,
    text,
    w_stem,
    w_time,
    conv_one,
    conv_two,
    kv_weight,
    w_query,
    w_output,
    w_head,
):
    dp_size = lax.axis_size("dp")
    mp_size = lax.axis_size("mp")
    n = dp_size * mp_size
    images, tokens, features = text.shape
    pixels = clean.shape[2]
    channels, width = w_query.shape
    span = TAPS * channels
    half = kv_weight.shape[0]
    own = 2 * width // dp_size
    rows = conv_one.shape[0] // n
    radices = radices_of(dp_size)
    orders = (
        order_of(radices),
        order_of(radices, turned=True),
        order_of(radices),
        order_of((dp_size,)),
    )
    kv_block = (own, half // (len(orders) - 2))
    turn = lambda x: jnp.transpose(x, (1, 0, 2))
    arrays = (
        turn(clean),
        turn(noise),
        turn(lowres),
        turn(aug_noise),
        text,
        kv_weight,
        w_stem,
        w_time,
        conv_one,
        conv_two,
        w_query,
        w_output,
        w_head,
    )
    vmem = pl.BlockSpec(memory_space=pltpu.VMEM)
    smem = pl.BlockSpec(memory_space=pltpu.SMEM)
    hbm = pl.BlockSpec(memory_space=pl.ANY)
    v = pltpu.VMEM
    dma = pltpu.SemaphoreType.DMA
    lines = pixels // S + 2
    conv_block = (rows, channels)
    one, two, kv, stats = pl.pallas_call(
        functools.partial(block_kernel, n, mp_size, orders),
        out_shape=(
            jax.ShapeDtypeStruct(conv_block, F32),
            jax.ShapeDtypeStruct(conv_block, F32),
            jax.ShapeDtypeStruct((own, half), F32),
            jax.ShapeDtypeStruct((1, 128), F32),
        ),
        in_specs=[smem] * 3 + [vmem] * 4 + [hbm] * 2 + [vmem] * (len(arrays) - 6),
        out_specs=(vmem,) * 4,
        scratch_shapes=[
            v((images, 8, 2 * channels), F32),
            v((images, tokens, 2 * width), BF16),
            v((images, tokens, 2 * width), BF16),
            v((width, HEADS * tokens), BF16),
            v((HEADS * tokens, width), BF16),
            v((HEADS * tokens, width), BF16),
            v((width, HEADS * tokens), BF16),
            v((width, channels), BF16),
            v((channels, width), BF16),
            v(((TAPS + 1) * span, 2 * channels), BF16),
            v(((TAPS + 1) * span, 2 * channels), BF16),
            v(((TAPS + 1) * span, 2 * channels), BF16),
            v((16, channels), F32),
            v((images, 8, pixels), F32),
            v((images, 8, pixels), F32),
            v((images, 4, 8, channels), F32),
            v((pixels, channels), F32),
            v((pixels + 16, channels), F32),
            v((images, lines, S, span), BF16),
            v((images, lines, S, span), BF16),
            v((images, lines, S, span), BF16),
            v((images, pixels, channels), F32),
            v((images, pixels, channels), F32),
            v((pixels, channels), BF16),
            v((pixels, channels), BF16),
            v((lines, S, channels), BF16),
            v((span, span), F32),
            v((HEADS * tokens, width), F32),
            v((HEADS * tokens, width), F32),
            v(conv_one.shape, F32),
            v(conv_one.shape, F32),
            v(text.shape, BF16),
            v(kv_weight.shape, BF16),
            dma((2,)),
            v((mp_size - 1,) + kv_weight.shape, BF16),
            dma((mp_size - 1,)),
            dma((mp_size - 1,)),
            v((1, 128), F32),
            v((n, 1, 128), F32),
            dma((n - 1,)),
            dma((n - 1,)),
            v((dp_size, own, features), BF16),
            v((mp_size, dp_size) + conv_block, BF16),
            v((mp_size, dp_size) + conv_block, BF16),
        ]
        + sum(
            (
                scratch_of(kv_block if c < len(orders) - 2 else conv_block, order, dp_size, mp_size)
                for c, order in enumerate(orders)
            ),
            [],
        ),
        compiler_params=pltpu.CompilerParams(
            collective_id=0, has_side_effects=True, vmem_limit_bytes=62 * 1024 * 1024
        ),
    )(timesteps, aug_levels, lengths, *arrays)
    conv_count = conv_one.shape[0] * conv_one.shape[1]
    kv_count = half * mp_size * 2 * width
    loss_count = images * n * clean.shape[1] * pixels
    one, two, kv, loss = pl.pallas_call(
        functools.partial(scale_kernel, conv_count, kv_count, loss_count),
        out_shape=(
            jax.ShapeDtypeStruct(conv_block, F32),
            jax.ShapeDtypeStruct(conv_block, F32),
            jax.ShapeDtypeStruct((own, half), F32),
            jax.ShapeDtypeStruct((1, 1), F32),
        ),
        in_specs=[vmem] * 4,
        out_specs=(vmem,) * 4,
    )(one, two, kv, stats)
    return (one, two, kv.T, loss.reshape(()))


def solution(mesh):
    return jax.shard_map(
        local,
        mesh=mesh,
        in_specs=(
            P(("dp", "mp"), None, None),
            P(("dp", "mp"), None, None),
            P(("dp", "mp"), None, None),
            P(("dp", "mp"), None, None),
            P(("dp", "mp")),
            P(("dp", "mp")),
            P(("dp", "mp")),
            P(("dp", "mp"), None, None),
            P(),
            P(),
            P(),
            P(),
            P("mp", None),
            P(),
            P(),
            P(),
        ),
        out_specs=(P(("dp", "mp"), None), P(("dp", "mp"), None), P("mp", "dp"), P()),
        check_vma=False,
    )
```
